32 devices in a mesh: batch: 1 (over z), row: 4 (over y), col: 8 (over x, core).
Axes of the slice: x: 4, y: 4, z: 1, core: 2. Of those that a mesh axis runs over, the one named last changes fastest.
The devices are a block of a 4x4x8 slice.
Arguments:
- lower_mat: bfloat16 [6144, 6144], P('row', 'col')
- rhs_mat: bfloat16 [6144, 768], P('row', ('batch', 'col'))
Outputs:
- output: bfloat16 [6144, 768], P('row', ('batch', 'col'))
All inputs are finite; a program needn't handle non-finite values.
Results may differ from the reference program's by a relative error of at most 0.001.
Values are sent between devices in bfloat16 or wider.
A program may use at most 768 MiB of HBM per device.

```python
import jax
import jax.numpy as jnp
from jax import lax

MAT_ORDER = 6144
BLOCK_SIZE = 256
RHS_COLS = 768
GRID_ROWS = 4
GRID_COLS = 8


def stored_to_global(positions, grid_size):
    per_device = MAT_ORDER // grid_size
    device_idx = positions // per_device
    local_pos = positions % per_device
    return ((local_pos // BLOCK_SIZE) * grid_size + device_idx) * BLOCK_SIZE + local_pos % BLOCK_SIZE


def setup_inputs(seed: int = 0, part: int = 0) -> dict:
    key_mat, key_rhs = jax.random.split(jax.random.key(seed))
    col_global = stored_to_global(jnp.arange(MAT_ORDER), GRID_COLS)

    def draw_rows(block_idx):
        row_global = stored_to_global(block_idx * BLOCK_SIZE + jnp.arange(BLOCK_SIZE), GRID_ROWS)
        draws = jax.random.normal(jax.random.fold_in(key_mat, block_idx), (BLOCK_SIZE, MAT_ORDER), jnp.float32)
        scaled = draws / jnp.sqrt((row_global + 1).astype(jnp.float32))[:, None]
        keep = col_global[None, :] <= row_global[:, None]
        return jnp.where(keep, scaled, 0.0).astype(jnp.bfloat16)

    lower_mat = lax.map(draw_rows, jnp.arange(MAT_ORDER // BLOCK_SIZE)).reshape(MAT_ORDER, MAT_ORDER)
    rhs_mat = jax.random.normal(jax.random.fold_in(key_rhs, part), (MAT_ORDER, RHS_COLS), jnp.float32).astype(jnp.bfloat16)
    return {"lower_mat": lower_mat, "rhs_mat": rhs_mat}


def reference(lower_mat, rhs_mat):
    total_blocks = MAT_ORDER // BLOCK_SIZE
    row_blocks = total_blocks // GRID_ROWS
    col_blocks = total_blocks // GRID_COLS
    rhs_global = rhs_mat.reshape(GRID_ROWS, row_blocks, BLOCK_SIZE, RHS_COLS).transpose(1, 0, 2, 3).reshape(MAT_ORDER, RHS_COLS)
    outputs = []
    for stored_block in range(total_blocks):
        global_block = (stored_block % row_blocks) * GRID_ROWS + stored_block // row_blocks
        width = (global_block + 1) * BLOCK_SIZE
        row_panel = lower_mat[stored_block * BLOCK_SIZE:(stored_block + 1) * BLOCK_SIZE]
        panel_global = row_panel.reshape(BLOCK_SIZE, GRID_COLS, col_blocks, BLOCK_SIZE).transpose(0, 2, 1, 3).reshape(BLOCK_SIZE, MAT_ORDER)
        block_sum = jnp.dot(panel_global[:, :width], rhs_global[:width], preferred_element_type=jnp.float32)
        outputs.append(block_sum.astype(jnp.bfloat16))
    return jnp.concatenate(outputs, axis=0)
```

```python
import functools

import jax
import jax.numpy as jnp
from jax import lax
from jax.experimental import pallas as pl
from jax.experimental.pallas import tpu as pltpu
from jax.sharding import PartitionSpec as P

BLOCK = 256
CORES = 2
F32, BF16 = jnp.float32, jnp.bfloat16


def kernel(ny, nx, nt, l_hbm, b_hbm, x_out, l_v, b_v, b_all, part, far_in, end_in,
           l_sem, lsend_sem, lrecv_sem, bload_sem, xsend_sem, ysend_sem, brecv_sem, psend_sem, far_sem, end_sem):
    cols = b_hbm.shape[0]
    y = lax.axis_index("row")
    c = lax.axis_index("col")
    x, j = c // CORES, c % CORES

    def at(yy, xx, jj=j):
        return {"row": yy, "col": CORES * xx + jj}

    def remote(src, dst, send, recv, dev):
        return pltpu.make_async_remote_copy(src_ref=src, dst_ref=dst, send_sem=send, recv_sem=recv, device_id=dev,
                                            device_id_type=pl.DeviceIdType.MESH)

    xr, xl = (x + 1) % nx, (x + nx - 1) % nx
    steps = [(t, p) for t in range(nt) for p in range(2)]

    load_b = pltpu.make_async_copy(b_hbm, b_v, bload_sem)
    load_b.start()

    def l_slice(t, core):
        return (pl.ds(2 * t * BLOCK, (2 * nt - 2 * t) * BLOCK), pl.ds(pl.multiple_of((2 * t + core) * BLOCK, BLOCK), BLOCK))

    def l_src(t):
        return l_hbm.at[pl.ds(2 * t * BLOCK, (2 * nt - 2 * t) * BLOCK), pl.ds(t * BLOCK, BLOCK)]

    load_l = [pltpu.make_async_copy(l_src(t), l_v.at[l_slice(t, j)], l_sem.at[t]) for t in range(nt)]
    for copy in load_l:
        copy.start()

    barrier = pltpu.get_barrier_semaphore()
    peers = [at(y, x, 1 - j)] + [at(y, (x + d) % nx) for d in range(1, nx)] + [at((y + d) % ny, x) for d in range(1, ny)]
    for dev in peers:
        pl.semaphore_signal(barrier, inc=1, device_id=dev, device_id_type=pl.DeviceIdType.MESH)

    load_b.wait()
    pl.semaphore_wait(barrier, len(peers))

    def b_block(m):
        return b_v.at[:, pl.ds(m * BLOCK, BLOCK)]

    s_own = y % 2
    chunk_p, chunk_q = x % 2, x // 2
    for m in range(2 * nt):
        t = m // 2
        xt = y // 2 + 2 * (m % 2)
        dst = b_all.at[t, chunk_p, chunk_q, s_own]

        @pl.when(xt != x)
        def _():
            remote(b_block(m), dst, xsend_sem.at[m], brecv_sem.at[t, chunk_p, chunk_q, s_own], at(y, xt)).start()

        @pl.when(xt == x)
        def _():
            pltpu.make_async_copy(b_block(m), dst, brecv_sem.at[t, chunk_p, chunk_q, s_own]).start()

    l_copies = [remote(l_src(t), l_v.at[l_slice(t, j)], lsend_sem.at[t], lrecv_sem.at[t], at(y, x, 1 - j)) for t in range(nt)]
    for copy in l_copies:
        copy.start()

    is_holder = (y // 2) == (x % 2)
    hx = 2 * (x % 2)
    out_dir = 2 * s_own - 1
    y_partner = hx + 1 - s_own
    y_outer = (y + ny + out_dir) % ny
    y_next = (y + ny - out_dir) % ny
    s_first = is_holder.astype(jnp.int32) * s_own + (1 - is_holder.astype(jnp.int32)) * (1 - s_own)

    def recv_b(t, p, q, s):
        r = b_all.at[t, p, q, s]
        return pltpu.make_async_copy(r, r, brecv_sem.at[t, p, q, s])

    def y_copy(t, p, q, s, which, yy):
        r = b_all.at[t, p, q, s]
        return remote(r, r, ysend_sem.at[t, p, q, which], brecv_sem.at[t, p, q, s], at(yy, x))

    def forward_b(t, p):
        for q in range(2):
            recv_b(t, p, q, s_first).wait()

            @pl.when(is_holder)
            def _():
                y_copy(t, p, q, s_own, 0, y_outer).start()
                y_copy(t, p, q, s_own, 1, y_partner).start()

            @pl.when(jnp.logical_not(is_holder))
            def _():
                y_copy(t, p, q, 1 - s_own, 0, y_outer_nh).start()

    y_outer_nh = (y + ny + 1 - 2 * s_own) % ny

    def compute(t, p):
        for q in range(2):
            recv_b(t, p, q, 1 - s_first).wait()
        if p == 0:
            load_l[t].wait()
            l_copies[t].wait_recv()
        for h in range(2):
            m = 2 * t + h
            acc = jnp.zeros((2 * cols, BLOCK), F32)
            for u in range(t + 1):
                for s in range(2):
                    lhs = b_all[u, p, :, s].reshape(2 * cols, BLOCK)
                    rhs = l_v[m * BLOCK:(m + 1) * BLOCK, (2 * u + s) * BLOCK:(2 * u + s + 1) * BLOCK]
                    acc += lax.dot_general(lhs, rhs, (((1,), (1,)), ((), ())), preferred_element_type=F32)
            part[t, p, :, h] = acc.reshape(2, cols, BLOCK)

    q_own = x // 2
    q_far = 1 - q_own
    q_r, q_l = xr // 2, xl // 2

    def far_copy(t, p, h):
        return remote(part.at[t, p, q_far, h], far_in.at[t, h], psend_sem.at[t, p, h], far_sem.at[t, h], at(y, xl if h else xr))

    def end_copy(t, p, side, h):
        q, dev = (q_l, xl) if side else (q_r, xr)
        return remote(part.at[t, p, q, h], end_in.at[t, side, h], psend_sem.at[t, p, 2 * side + h], end_sem.at[t, side, h], at(y, dev))

    def first_sends(t, p):
        @pl.when(x % 2 == p)
        def _():
            far_copy(t, p, 0).start()
            far_copy(t, p, 1).start()

        @pl.when(x % 2 != p)
        def _():
            end_copy(t, p, 0, 1).start()
            end_copy(t, p, 1, 0).start()

    def merge(t, p):
        @pl.when(x % 2 != p)
        def _():
            for h, q in ((0, q_r), (1, q_l)):
                pltpu.make_async_copy(far_in.at[t, h], far_in.at[t, h], far_sem.at[t, h]).wait()
                part[t, p, q, h] += far_in[t, h]
                end_copy(t, p, h, h).start()

    def finish(t, p):
        @pl.when(x % 2 == p)
        def _():
            for h in range(2):
                for side in range(2):
                    r = end_in.at[t, side, h]
                    pltpu.make_async_copy(r, r, end_sem.at[t, side, h]).wait()
                total = part[t, p, q_own, h] + (end_in[t, 0, h] + end_in[t, 1, h])
                m = 2 * t + h
                x_out[:, m * BLOCK:(m + 1) * BLOCK] = total.astype(BF16)

    for n, (t, p) in enumerate(steps):
        forward_b(t, p)
        compute(t, p)
        first_sends(t, p)
        if n >= 1:
            merge(*steps[n - 1])
        if n >= 3:
            finish(*steps[n - 3])
    merge(*steps[-1])
    for n in range(len(steps) - 3, len(steps)):
        finish(*steps[n])

    for m in range(2 * nt):
        xt = y // 2 + 2 * (m % 2)

        @pl.when(xt != x)
        def _():
            remote(b_block(m), b_block(m), xsend_sem.at[m], xsend_sem.at[m], at(y, xt)).wait_send()
    for copy in l_copies:
        copy.wait_send()
    for t, p in steps:
        for q in range(2):
            @pl.when(is_holder)
            def _():
                y_copy(t, p, q, s_own, 0, y_outer).wait_send()
                y_copy(t, p, q, s_own, 1, y_partner).wait_send()

            @pl.when(jnp.logical_not(is_holder))
            def _():
                y_copy(t, p, q, 1 - s_own, 0, y_outer_nh).wait_send()

        @pl.when(x % 2 == p)
        def _():
            far_copy(t, p, 0).wait_send()
            far_copy(t, p, 1).wait_send()

        @pl.when(x % 2 != p)
        def _():
            for side in range(2):
                for h in range(2):
                    end_copy(t, p, side, h).wait_send()


def solution(mesh):
    ny = mesh.shape["row"]
    nx = mesh.shape["col"] // CORES

    def local_product(lower_loc, rhs_loc):
        rows, width = lower_loc.shape
        cols = rhs_loc.shape[1]
        nt = width // BLOCK
        dma = pltpu.SemaphoreType.DMA
        return pl.pallas_call(
            functools.partial(kernel, ny, nx, nt),
            out_shape=jax.ShapeDtypeStruct((cols, rows), BF16),
            in_specs=[pl.BlockSpec(memory_space=pl.ANY)] * 2,
            out_specs=pl.BlockSpec(memory_space=pltpu.VMEM),
            scratch_shapes=[
                pltpu.VMEM((rows, CORES * width), BF16),
                pltpu.VMEM((cols, rows), BF16),
                pltpu.VMEM((nt, 2, 2, 2, cols, BLOCK), BF16),
                pltpu.VMEM((nt, 2, 2, 2, cols, BLOCK), F32),
                pltpu.VMEM((nt, 2, cols, BLOCK), F32),
                pltpu.VMEM((nt, 2, 2, cols, BLOCK), F32),
                dma((nt,)), dma((nt,)), dma((nt,)), dma, dma((2 * nt,)), dma((nt, 2, 2, 2)), dma((nt, 2, 2, 2)),
                dma((nt, 2, 4)), dma((nt, 2)), dma((nt, 2, 2)),
            ],
            compiler_params=pltpu.CompilerParams(collective_id=0, has_side_effects=True),
        )(lower_loc, rhs_loc.T).T

    return jax.shard_map(local_product, mesh=mesh, in_specs=(P("row", "col"), P("row", ("batch", "col"))),
                         out_specs=P("row", ("batch", "col")), check_vma=False)
```

```python
import functools

import jax
import jax.numpy as jnp
from jax import lax
from jax.experimental import pallas as pl
from jax.experimental.pallas import tpu as pltpu
from jax.sharding import PartitionSpec as P

BLOCK = 256
CORES = 2
F32, BF16 = jnp.float32, jnp.bfloat16


def kernel(ny, nx, nt, l_hbm, b_hbm, x_out, l_v, b_v, b_all, part, far_in, end_in,
           l_sem, lsend_sem, lrecv_sem, bload_sem, xsend_sem, ysend_sem, brecv_sem, psend_sem, far_sem, end_sem):
    cols = b_hbm.shape[0]
    y = lax.axis_index("row")
    c = lax.axis_index("col")
    x, j = c // CORES, c % CORES

    def at(yy, xx, jj=j):
        return {"row": yy, "col": CORES * xx + jj}

    def remote(src, dst, send, recv, dev):
        return pltpu.make_async_remote_copy(src_ref=src, dst_ref=dst, send_sem=send, recv_sem=recv, device_id=dev,
                                            device_id_type=pl.DeviceIdType.MESH)

    xr, xl = (x + 1) % nx, (x + nx - 1) % nx
    steps = [(t, p) for t in range(nt) for p in range(2)]

    load_b = pltpu.make_async_copy(b_hbm, b_v, bload_sem)
    load_b.start()

    def l_slice(t, core):
        return (pl.ds(2 * t * BLOCK, (2 * nt - 2 * t) * BLOCK), pl.ds(pl.multiple_of((2 * t + core) * BLOCK, BLOCK), BLOCK))

    def l_src(t):
        return l_hbm.at[pl.ds(2 * t * BLOCK, (2 * nt - 2 * t) * BLOCK), pl.ds(t * BLOCK, BLOCK)]

    load_l = [pltpu.make_async_copy(l_src(t), l_v.at[l_slice(t, j)], l_sem.at[t]) for t in range(nt)]
    for copy in load_l:
        copy.start()

    barrier = pltpu.get_barrier_semaphore()
    peers = [at(y, x, 1 - j)] + [at(y, (x + d) % nx) for d in range(1, nx)] + [at((y + d) % ny, x) for d in range(1, ny)]
    for dev in peers:
        pl.semaphore_signal(barrier, inc=1, device_id=dev, device_id_type=pl.DeviceIdType.MESH)

    load_b.wait()
    pl.semaphore_wait(barrier, len(peers))

    def b_block(m):
        return b_v.at[:, pl.ds(m * BLOCK, BLOCK)]

    s_own = y % 2
    chunk_p, chunk_q = x % 2, x // 2
    for m in range(2 * nt):
        t = m // 2
        xt = y // 2 + 2 * (m % 2)
        dst = b_all.at[t, chunk_p, chunk_q, s_own]

        @pl.when(xt != x)
        def _():
            remote(b_block(m), dst, xsend_sem.at[m], brecv_sem.at[t, chunk_p, chunk_q, s_own], at(y, xt)).start()

        @pl.when(xt == x)
        def _():
            pltpu.make_async_copy(b_block(m), dst, brecv_sem.at[t, chunk_p, chunk_q, s_own]).start()

    l_copies = [remote(l_src(t), l_v.at[l_slice(t, j)], lsend_sem.at[t], lrecv_sem.at[t], at(y, x, 1 - j)) for t in range(nt)]
    for copy in l_copies:
        copy.start()

    is_holder = (y // 2) == (x % 2)
    hx = 2 * (x % 2)
    out_dir = 2 * s_own - 1
    y_partner = hx + 1 - s_own
    y_outer = (y + ny + out_dir) % ny
    y_next = (y + ny - out_dir) % ny
    s_first = is_holder.astype(jnp.int32) * s_own + (1 - is_holder.astype(jnp.int32)) * (1 - s_own)

    def recv_b(t, p, q, s):
        r = b_all.at[t, p, q, s]
        return pltpu.make_async_copy(r, r, brecv_sem.at[t, p, q, s])

    def y_copy(t, p, q, s, which, yy):
        r = b_all.at[t, p, q, s]
        return remote(r, r, ysend_sem.at[t, p, q, which], brecv_sem.at[t, p, q, s], at(yy, x))

    def forward_held(t, p):
        @pl.when(is_holder)
        def _():
            for q in range(2):
                recv_b(t, p, q, s_own).wait()
                y_copy(t, p, q, s_own, 0, y_outer).start()
                y_copy(t, p, q, s_own, 1, y_partner).start()

    def forward_passed(t, p):
        @pl.when(jnp.logical_not(is_holder))
        def _():
            for q in range(2):
                recv_b(t, p, q, 1 - s_own).wait()
                y_copy(t, p, q, 1 - s_own, 0, y_outer_nh).start()

    y_outer_nh = (y + ny + 1 - 2 * s_own) % ny

    def compute(t, p):
        for q in range(2):
            recv_b(t, p, q, 1 - s_first).wait()
        if p == 0:
            load_l[t].wait()
            l_copies[t].wait_recv()
        for h in range(2):
            m = 2 * t + h
            acc = jnp.zeros((2 * cols, BLOCK), F32)
            for u in range(t + 1):
                for s in range(2):
                    lhs = b_all[u, p, :, s].reshape(2 * cols, BLOCK)
                    rhs = l_v[m * BLOCK:(m + 1) * BLOCK, (2 * u + s) * BLOCK:(2 * u + s + 1) * BLOCK]
                    acc += lax.dot_general(lhs, rhs, (((1,), (1,)), ((), ())), preferred_element_type=F32)
            part[t, p, :, h] = acc.reshape(2, cols, BLOCK)

    q_own = x // 2
    q_far = 1 - q_own
    q_r, q_l = xr // 2, xl // 2

    def far_copy(t, p, h):
        return remote(part.at[t, p, q_far, h], far_in.at[t, h], psend_sem.at[t, p, h], far_sem.at[t, h], at(y, xl if h else xr))

    def end_copy(t, p, side, h):
        q, dev = (q_l, xl) if side else (q_r, xr)
        return remote(part.at[t, p, q, h], end_in.at[t, side, h], psend_sem.at[t, p, 2 * side + h], end_sem.at[t, side, h], at(y, dev))

    def first_sends(t, p):
        @pl.when(x % 2 == p)
        def _():
            far_copy(t, p, 0).start()
            far_copy(t, p, 1).start()

        @pl.when(x % 2 != p)
        def _():
            end_copy(t, p, 0, 1).start()
            end_copy(t, p, 1, 0).start()

    def merge(t, p):
        @pl.when(x % 2 != p)
        def _():
            for h, q in ((0, q_r), (1, q_l)):
                pltpu.make_async_copy(far_in.at[t, h], far_in.at[t, h], far_sem.at[t, h]).wait()
                part[t, p, q, h] += far_in[t, h]
                end_copy(t, p, h, h).start()

    def finish(t, p):
        @pl.when(x % 2 == p)
        def _():
            for h in range(2):
                for side in range(2):
                    r = end_in.at[t, side, h]
                    pltpu.make_async_copy(r, r, end_sem.at[t, side, h]).wait()
                total = part[t, p, q_own, h] + (end_in[t, 0, h] + end_in[t, 1, h])
                m = 2 * t + h
                x_out[:, m * BLOCK:(m + 1) * BLOCK] = total.astype(BF16)

    for t, p in steps:
        forward_held(t, p)
    forward_passed(*steps[0])
    for n, (t, p) in enumerate(steps):
        if n + 1 < len(steps):
            forward_passed(*steps[n + 1])
        compute(t, p)
        first_sends(t, p)
        if n >= 1:
            merge(*steps[n - 1])
        if n >= 3:
            finish(*steps[n - 3])
    merge(*steps[-1])
    for n in range(len(steps) - 3, len(steps)):
        finish(*steps[n])

    for m in range(2 * nt):
        xt = y // 2 + 2 * (m % 2)

        @pl.when(xt != x)
        def _():
            remote(b_block(m), b_block(m), xsend_sem.at[m], xsend_sem.at[m], at(y, xt)).wait_send()
    for copy in l_copies:
        copy.wait_send()
    for t, p in steps:
        for q in range(2):
            @pl.when(is_holder)
            def _():
                y_copy(t, p, q, s_own, 0, y_outer).wait_send()
                y_copy(t, p, q, s_own, 1, y_partner).wait_send()

            @pl.when(jnp.logical_not(is_holder))
            def _():
                y_copy(t, p, q, 1 - s_own, 0, y_outer_nh).wait_send()

        @pl.when(x % 2 == p)
        def _():
            far_copy(t, p, 0).wait_send()
            far_copy(t, p, 1).wait_send()

        @pl.when(x % 2 != p)
        def _():
            for side in range(2):
                for h in range(2):
                    end_copy(t, p, side, h).wait_send()


def solution(mesh):
    ny = mesh.shape["row"]
    nx = mesh.shape["col"] // CORES

    def local_product(lower_loc, rhs_loc):
        rows, width = lower_loc.shape
        cols = rhs_loc.shape[1]
        nt = width // BLOCK
        dma = pltpu.SemaphoreType.DMA
        return pl.pallas_call(
            functools.partial(kernel, ny, nx, nt),
            out_shape=pltpu.VMEM((cols, rows), BF16),
            in_specs=[pl.BlockSpec(memory_space=pl.ANY)] * 2,
            out_specs=pl.BlockSpec(memory_space=pltpu.VMEM),
            scratch_shapes=[
                pltpu.VMEM((rows, CORES * width), BF16),
                pltpu.VMEM((cols, rows), BF16),
                pltpu.VMEM((nt, 2, 2, 2, cols, BLOCK), BF16),
                pltpu.VMEM((nt, 2, 2, 2, cols, BLOCK), F32),
                pltpu.VMEM((nt, 2, cols, BLOCK), F32),
                pltpu.VMEM((nt, 2, 2, cols, BLOCK), F32),
                dma((nt,)), dma((nt,)), dma((nt,)), dma, dma((2 * nt,)), dma((nt, 2, 2, 2)), dma((nt, 2, 2, 2)),
                dma((nt, 2, 4)), dma((nt, 2)), dma((nt, 2, 2)),
            ],
            compiler_params=pltpu.CompilerParams(collective_id=0, has_side_effects=True),
        )(lower_loc, rhs_loc.T).T

    return jax.shard_map(local_product, mesh=mesh, in_specs=(P("row", "col"), P("row", ("batch", "col"))),
                         out_specs=P("row", ("batch", "col")), check_vma=False)
```

```python
import functools

import jax
import jax.numpy as jnp
from jax import lax
from jax.experimental import pallas as pl
from jax.experimental.pallas import tpu as pltpu
from jax.sharding import PartitionSpec as P

BLOCK = 256
CORES = 2
F32, BF16 = jnp.float32, jnp.bfloat16


def kernel(ny, nx, nt, l_hbm, b_hbm, x_out, l_v, b_v, b_col, b_all, part, far_in, end_in, l_sem, lsend, lrecv, bload, gsend, grecv,
           xsend, ysend, brecv, psend, far_sem, end_sem):
    cols = b_hbm.shape[0]
    y = lax.axis_index("row")
    c = lax.axis_index("col")
    x, j = c // CORES, c % CORES

    def at(yy, xx, jj=j):
        return {"row": yy, "col": CORES * xx + jj}

    def remote(src, dst, send, recv, dev):
        return pltpu.make_async_remote_copy(src_ref=src, dst_ref=dst, send_sem=send, recv_sem=recv, device_id=dev,
                                            device_id_type=pl.DeviceIdType.MESH)

    def landed(ref, sem):
        pltpu.make_async_copy(ref, ref, sem).wait()

    xr, xl = (x + 1) % nx, (x + nx - 1) % nx
    yu, yd = (y + 1) % ny, (y + ny - 1) % ny
    p_end, p_mid = x % 2, 1 - x % 2

    load_b = pltpu.make_async_copy(b_hbm, b_v, bload)
    load_b.start()

    def l_slice(t, core):
        return (pl.ds(2 * t * BLOCK, (2 * nt - 2 * t) * BLOCK), pl.ds(pl.multiple_of((2 * t + core) * BLOCK, BLOCK), BLOCK))

    def l_src(t):
        return l_hbm.at[pl.ds(2 * t * BLOCK, (2 * nt - 2 * t) * BLOCK), pl.ds(t * BLOCK, BLOCK)]

    load_l = [pltpu.make_async_copy(l_src(t), l_v.at[l_slice(t, j)], l_sem.at[t]) for t in range(nt)]
    for copy in load_l:
        copy.start()

    barrier = pltpu.get_barrier_semaphore()
    peers = [at(y, x, 1 - j)] + [at(y, (x + d) % nx) for d in range(1, nx)] + [at(yu, x), at(yd, x)]
    for dev in peers:
        pl.semaphore_signal(barrier, inc=1, device_id=dev, device_id_type=pl.DeviceIdType.MESH)
    load_b.wait()
    pl.semaphore_wait(barrier, len(peers))

    def b_block(m):
        return b_v.at[:, pl.ds(m * BLOCK, BLOCK)]

    s_own = y % 2
    chunk_p, chunk_q = x % 2, x // 2

    def gather_copy(m, yy, i):
        k = ny * m + y
        return remote(b_block(m), b_col.at[k], gsend.at[i], grecv.at[k], at(yy, x))

    def pass_copy(m, y_from, y_to, i):
        r = b_col.at[ny * m + y_from]
        return remote(r, r, gsend.at[i], grecv.at[ny * m + y_from], at(y_to, x))

    gathers = [gather_copy(0, yu, 0), gather_copy(1, yd, 1), gather_copy(1, yu, 2), gather_copy(0, yd, 3)]
    passes = [pass_copy(0, yd, yu, 4), pass_copy(1, yu, yd, 5)]

    def place_copy(m, d):
        yy = (y + d) % ny
        src = b_col.at[ny * m + yy] if d else b_block(m)
        dst, sem = b_all.at[0, chunk_p, chunk_q, yy % 2], brecv.at[0, chunk_p, chunk_q, yy % 2]
        xt = yy // 2 + 2 * m
        return xt, (lambda: remote(src, dst, gsend.at[6 + ny * m + d], sem, at(y, xt))), (lambda: pltpu.make_async_copy(src, dst, sem))

    def came(m, d):
        k = ny * m + (y + d) % ny
        landed(b_col.at[k], grecv.at[k])

    def place(m, d):
        xt, away, here = place_copy(m, d)

        @pl.when(xt != x)
        def _():
            away().start()

        @pl.when(xt == x)
        def _():
            here().start()

    def x_copy(m):
        xt = y // 2 + 2 * (m % 2)
        dst, sem = b_all.at[m // 2, chunk_p, chunk_q, s_own], brecv.at[m // 2, chunk_p, chunk_q, s_own]
        return xt, (lambda: remote(b_block(m), dst, xsend.at[m], sem, at(y, xt))), (lambda: pltpu.make_async_copy(b_block(m), dst, sem))

    def x_first(t):
        for m in (2 * t, 2 * t + 1):
            xt, away, here = x_copy(m)

            @pl.when(xt != x)
            def _():
                away().start()

            @pl.when(xt == x)
            def _():
                here().start()

    is_holder = (y // 2) == (x % 2)
    hx = 2 * (x % 2)
    y_partner = hx + 1 - s_own
    y_outer = (y + ny + 2 * s_own - 1) % ny
    y_next = (y + ny + 1 - 2 * s_own) % ny
    held = is_holder.astype(jnp.int32)
    s_first = held * s_own + (1 - held) * (1 - s_own)

    def y_copy(t, p, q, s, which, yy):
        r = b_all.at[t, p, q, s]
        return remote(r, r, ysend.at[t, p, q, which], brecv.at[t, p, q, s], at(yy, x))

    def b_came(t, p, q, s):
        landed(b_all.at[t, p, q, s], brecv.at[t, p, q, s])

    def forward_held(t):
        @pl.when(is_holder)
        def _():
            for p in (p_end, p_mid):
                for q in range(2):
                    b_came(t, p, q, s_own)
                    y_copy(t, p, q, s_own, 0, y_outer).start()
                    y_copy(t, p, q, s_own, 1, y_partner).start()

    def forward_passed(t, p):
        @pl.when(jnp.logical_not(is_holder))
        def _():
            for q in range(2):
                b_came(t, p, q, 1 - s_own)
                y_copy(t, p, q, 1 - s_own, 0, y_next).start()

    def compute(t, role):
        p = (p_end, p_mid)[role]
        for q in range(2):
            for s in range(2) if t == 0 else (1 - s_first,):
                b_came(t, p, q, s)
        if role == 0:
            load_l[t].wait()
            l_copies[t].wait_recv()
        for h in range(2):
            m = 2 * t + h
            acc = jnp.zeros((2 * cols, BLOCK), F32)
            for u in range(t + 1):
                for s in range(2):
                    lhs = b_all[u, p, :, s].reshape(2 * cols, BLOCK)
                    rhs = l_v[m * BLOCK:(m + 1) * BLOCK, (2 * u + s) * BLOCK:(2 * u + s + 1) * BLOCK]
                    acc += lax.dot_general(lhs, rhs, (((1,), (1,)), ((), ())), preferred_element_type=F32)
            part[t, role, :, h] = acc.reshape(2, cols, BLOCK)

    q_own = x // 2

    def far_copy(t, h):
        return remote(part.at[t, 0, 1 - q_own, h], far_in.at[t, h], psend.at[t, h], far_sem.at[t, h], at(y, xl if h else xr))

    def end_copy(t, side, h):
        xx = xl if side else xr
        return remote(part.at[t, 1, xx // 2, h], end_in.at[t, side, h], psend.at[t, 2 + 2 * side + h], end_sem.at[t, side, h], at(y, xx))

    def ends(t):
        compute(t, 0)
        far_copy(t, 0).start()
        far_copy(t, 1).start()

    def middles(t):
        compute(t, 1)
        end_copy(t, 0, 1).start()
        end_copy(t, 1, 0).start()

    def merge(t):
        for h, xx in ((0, xr), (1, xl)):
            landed(far_in.at[t, h], far_sem.at[t, h])
            part[t, 1, xx // 2, h] += far_in[t, h]
            end_copy(t, h, h).start()

    def finish(t, h):
        for side in range(2):
            landed(end_in.at[t, side, h], end_sem.at[t, side, h])
        m = 2 * t + h
        x_out[:, m * BLOCK:(m + 1) * BLOCK] = (part[t, 0, q_own, h] + (end_in[t, 0, h] + end_in[t, 1, h])).astype(BF16)

    l_copies = [remote(l_src(t), l_v.at[l_slice(t, j)], lsend.at[t], lrecv.at[t], at(y, x, 1 - j)) for t in range(nt)]
    for copy in gathers:
        copy.start()
    place(0, 0)
    place(1, 0)
    x_first(1)
    for copy in l_copies:
        copy.start()
    came(0, ny - 1)
    passes[0].start()
    place(0, ny - 1)
    came(1, 1)
    passes[1].start()
    place(1, 1)
    came(1, ny - 1)
    place(1, ny - 1)
    came(0, 1)
    place(0, 1)
    for m in range(2):
        came(m, 2)
        place(m, 2)
    for t in range(2, nt):
        x_first(t)
    forward_held(1)
    ends(0)
    middles(0)
    forward_passed(1, p_end)
    forward_passed(1, p_mid)
    merge(0)
    forward_held(2)
    ends(1)
    middles(1)
    forward_passed(2, p_end)
    forward_passed(2, p_mid)
    merge(1)
    for h in range(2):
        finish(0, h)
    ends(2)
    middles(2)
    merge(2)
    for h in range(2):
        finish(1, h)

    for copy in gathers + passes + l_copies:
        copy.wait_send()
    for m in range(2):
        for d in range(ny):
            xt, away, _ = place_copy(m, d)

            @pl.when(xt != x)
            def _():
                away().wait_send()
    for m in range(2, 2 * nt):
        xt, away, _ = x_copy(m)

        @pl.when(xt != x)
        def _():
            away().wait_send()
    for t in range(1, nt):
        for p in range(2):
            for q in range(2):
                @pl.when(is_holder)
                def _():
                    y_copy(t, p, q, s_own, 0, y_outer).wait_send()
                    y_copy(t, p, q, s_own, 1, y_partner).wait_send()

                @pl.when(jnp.logical_not(is_holder))
                def _():
                    y_copy(t, p, q, 1 - s_own, 0, y_next).wait_send()
    for t in range(nt):
        for h in range(2):
            far_copy(t, h).wait_send()
            end_copy(t, 1 - h, h).wait_send()
    for t in range(nt - 1):
        for h in range(2):
            end_copy(t, h, h).wait_send()
    for h in range(2):
        finish(nt - 1, h)
    for h in range(2):
        end_copy(nt - 1, h, h).wait_send()


def solution(mesh):
    ny = mesh.shape["row"]
    nx = mesh.shape["col"] // CORES

    def local_product(lower_loc, rhs_loc):
        rows, width = lower_loc.shape
        cols = rhs_loc.shape[1]
        nt = width // BLOCK
        dma = pltpu.SemaphoreType.DMA
        return pl.pallas_call(
            functools.partial(kernel, ny, nx, nt),
            out_shape=pltpu.VMEM((cols, rows), BF16),
            in_specs=[pl.BlockSpec(memory_space=pl.ANY)] * 2,
            out_specs=pl.BlockSpec(memory_space=pltpu.VMEM),
            scratch_shapes=[
                pltpu.VMEM((rows, CORES * width), BF16),
                pltpu.VMEM((cols, rows), BF16),
                pltpu.VMEM((2 * ny, cols, BLOCK), BF16),
                pltpu.VMEM((nt, 2, 2, 2, cols, BLOCK), BF16),
                pltpu.VMEM((nt, 2, 2, 2, cols, BLOCK), F32),
                pltpu.VMEM((nt, 2, cols, BLOCK), F32),
                pltpu.VMEM((nt, 2, 2, cols, BLOCK), F32),
                dma((nt,)), dma((nt,)), dma((nt,)), dma, dma((6 + 2 * ny,)), dma((2 * ny,)), dma((2 * nt,)),
                dma((nt, 2, 2, 2)), dma((nt, 2, 2, 2)), dma((nt, 6)), dma((nt, 2)), dma((nt, 2, 2)),
            ],
            compiler_params=pltpu.CompilerParams(collective_id=0, has_side_effects=True),
        )(lower_loc, rhs_loc.T).T

    return jax.shard_map(local_product, mesh=mesh, in_specs=(P("row", "col"), P("row", ("batch", "col"))),
                         out_specs=P("row", ("batch", "col")), check_vma=False)
```

```python
import functools

import jax
import jax.numpy as jnp
from jax import lax
from jax.experimental import pallas as pl
from jax.experimental.pallas import tpu as pltpu
from jax.sharding import PartitionSpec as P

ORDER = (
    "g", "p0", "x1", "L", "a01", "a03", "a11", "a13", "x2", "a02", "a12", "h1", "E0", "M0", "h2", "fe1",
    "fm1", "G0", "E1", "M1", "fe2", "fm2", "E2", "M2", "G1", "F0", "G2", "F1",
)
BLOCK = 256
CORES = 2
F32, BF16 = jnp.float32, jnp.bfloat16


def kernel(ny, nx, nt, l_hbm, b_hbm, x_out, l_v, b_v, b_col, b_all, part, far_in, end_in, l_sem, lsend, lrecv, bload, gsend, grecv,
           xsend, ysend, brecv, psend, far_sem, end_sem):
    cols = b_hbm.shape[0]
    y = lax.axis_index("row")
    c = lax.axis_index("col")
    x, j = c // CORES, c % CORES

    def at(yy, xx, jj=j):
        return {"row": yy, "col": CORES * xx + jj}

    def remote(src, dst, send, recv, dev):
        return pltpu.make_async_remote_copy(src_ref=src, dst_ref=dst, send_sem=send, recv_sem=recv, device_id=dev,
                                            device_id_type=pl.DeviceIdType.MESH)

    def landed(ref, sem):
        pltpu.make_async_copy(ref, ref, sem).wait()

    xr, xl = (x + 1) % nx, (x + nx - 1) % nx
    yu, yd = (y + 1) % ny, (y + ny - 1) % ny
    p_end, p_mid = x % 2, 1 - x % 2

    load_b = pltpu.make_async_copy(b_hbm, b_v, bload)
    load_b.start()

    def l_slice(t, core):
        return (pl.ds(2 * t * BLOCK, (2 * nt - 2 * t) * BLOCK), pl.ds(pl.multiple_of((2 * t + core) * BLOCK, BLOCK), BLOCK))

    def l_src(t):
        return l_hbm.at[pl.ds(2 * t * BLOCK, (2 * nt - 2 * t) * BLOCK), pl.ds(t * BLOCK, BLOCK)]

    load_l = [pltpu.make_async_copy(l_src(t), l_v.at[l_slice(t, j)], l_sem.at[t]) for t in range(nt)]
    for copy in load_l:
        copy.start()

    barrier = pltpu.get_barrier_semaphore()
    peers = [at(y, x, 1 - j)] + [at(y, (x + d) % nx) for d in range(1, nx)] + [at(yu, x), at(yd, x)]
    for dev in peers:
        pl.semaphore_signal(barrier, inc=1, device_id=dev, device_id_type=pl.DeviceIdType.MESH)
    load_b.wait()
    pl.semaphore_wait(barrier, len(peers))

    def b_block(m):
        return b_v.at[:, pl.ds(m * BLOCK, BLOCK)]

    s_own = y % 2
    chunk_p, chunk_q = x % 2, x // 2

    def gather_copy(m, yy, i):
        k = ny * m + y
        return remote(b_block(m), b_col.at[k], gsend.at[i], grecv.at[k], at(yy, x))

    def pass_copy(m, y_from, y_to, i):
        r = b_col.at[ny * m + y_from]
        return remote(r, r, gsend.at[i], grecv.at[ny * m + y_from], at(y_to, x))

    gathers = [gather_copy(0, yu, 0), gather_copy(0, yd, 1), gather_copy(1, yu, 2), gather_copy(1, yd, 3)]
    passes = [pass_copy(1, yd, yu, 4), pass_copy(0, yu, yd, 5)]

    def place_copy(m, d):
        yy = (y + d) % ny
        src = b_col.at[ny * m + yy] if d else b_block(m)
        dst, sem = b_all.at[0, chunk_p, chunk_q, yy % 2], brecv.at[0, chunk_p, chunk_q, yy % 2]
        xt = yy // 2 + 2 * m
        return xt, (lambda: remote(src, dst, gsend.at[6 + ny * m + d], sem, at(y, xt))), (lambda: pltpu.make_async_copy(src, dst, sem))

    def came(m, d):
        k = ny * m + (y + d) % ny
        landed(b_col.at[k], grecv.at[k])

    def place(m, d):
        xt, away, here = place_copy(m, d)

        @pl.when(xt != x)
        def _():
            away().start()

        @pl.when(xt == x)
        def _():
            here().start()

    def x_copy(m):
        xt = y // 2 + 2 * (m % 2)
        dst, sem = b_all.at[m // 2, chunk_p, chunk_q, s_own], brecv.at[m // 2, chunk_p, chunk_q, s_own]
        return xt, (lambda: remote(b_block(m), dst, xsend.at[m], sem, at(y, xt))), (lambda: pltpu.make_async_copy(b_block(m), dst, sem))

    def x_first(t):
        for m in (2 * t, 2 * t + 1):
            xt, away, here = x_copy(m)

            @pl.when(xt != x)
            def _():
                away().start()

            @pl.when(xt == x)
            def _():
                here().start()

    is_holder = (y // 2) == (x % 2)
    hx = 2 * (x % 2)
    y_partner = hx + 1 - s_own
    y_outer = (y + ny + 2 * s_own - 1) % ny
    y_next = (y + ny + 1 - 2 * s_own) % ny
    held = is_holder.astype(jnp.int32)
    s_first = held * s_own + (1 - held) * (1 - s_own)

    def y_copy(t, p, q, s, which, yy):
        r = b_all.at[t, p, q, s]
        return remote(r, r, ysend.at[t, p, q, which], brecv.at[t, p, q, s], at(yy, x))

    def b_came(t, p, q, s):
        landed(b_all.at[t, p, q, s], brecv.at[t, p, q, s])

    def forward_held(t):
        @pl.when(is_holder)
        def _():
            for p in (p_end, p_mid):
                for q in range(2):
                    b_came(t, p, q, s_own)
                    y_copy(t, p, q, s_own, 0, y_outer).start()
                    y_copy(t, p, q, s_own, 1, y_partner).start()

    def forward_passed(t, p):
        @pl.when(jnp.logical_not(is_holder))
        def _():
            for q in range(2):
                b_came(t, p, q, 1 - s_own)
                y_copy(t, p, q, 1 - s_own, 0, y_next).start()

    def compute(t, role):
        p = (p_end, p_mid)[role]
        if t == 0:
            for s in range(2):
                @pl.when(CORES * x + s <= y + ny)
                def _():
                    for q in range(2):
                        b_came(t, p, q, s)
        else:
            for q in range(2):
                b_came(t, p, q, 1 - s_first)
        if t == 1:
            for s in range(2):
                @pl.when(CORES * x + s > y + ny)
                def _():
                    for q in range(2):
                        b_came(0, p, q, s)
        if role == 0:
            load_l[t].wait()
            l_copies[t].wait_recv()
        for h in range(2):
            m = 2 * t + h
            if t == 0:
                part[t, role, :, h] = jnp.zeros((2, cols, BLOCK), F32)
                for s in range(2):
                    @pl.when(CORES * x + s <= y + ny * h)
                    def _():
                        lhs = b_all[0, p, :, s].reshape(2 * cols, BLOCK)
                        rhs = l_v[m * BLOCK:(m + 1) * BLOCK, s * BLOCK:(s + 1) * BLOCK]
                        acc = lax.dot_general(lhs, rhs, (((1,), (1,)), ((), ())), preferred_element_type=F32)
                        part[t, role, :, h] += acc.reshape(2, cols, BLOCK)
                continue
            acc = jnp.zeros((2 * cols, BLOCK), F32)
            for u in range(t + 1):
                for s in range(2):
                    lhs = b_all[u, p, :, s].reshape(2 * cols, BLOCK)
                    rhs = l_v[m * BLOCK:(m + 1) * BLOCK, (2 * u + s) * BLOCK:(2 * u + s + 1) * BLOCK]
                    acc += lax.dot_general(lhs, rhs, (((1,), (1,)), ((), ())), preferred_element_type=F32)
            part[t, role, :, h] = acc.reshape(2, cols, BLOCK)

    q_own = x // 2

    def far_copy(t, h):
        return remote(part.at[t, 0, 1 - q_own, h], far_in.at[t, h], psend.at[t, h], far_sem.at[t, h], at(y, xl if h else xr))

    def end_copy(t, side, h):
        xx = xl if side else xr
        return remote(part.at[t, 1, xx // 2, h], end_in.at[t, side, h], psend.at[t, 2 + 2 * side + h], end_sem.at[t, side, h], at(y, xx))

    def ends(t):
        compute(t, 0)
        far_copy(t, 0).start()
        far_copy(t, 1).start()

    def middles(t):
        compute(t, 1)
        end_copy(t, 0, 1).start()
        end_copy(t, 1, 0).start()

    def merge(t):
        for h, xx in ((0, xr), (1, xl)):
            landed(far_in.at[t, h], far_sem.at[t, h])
            part[t, 1, xx // 2, h] += far_in[t, h]
            end_copy(t, h, h).start()

    def finish(t, h):
        for side in range(2):
            landed(end_in.at[t, side, h], end_sem.at[t, side, h])
        m = 2 * t + h
        x_out[:, m * BLOCK:(m + 1) * BLOCK] = (part[t, 0, q_own, h] + (end_in[t, 0, h] + end_in[t, 1, h])).astype(BF16)

    l_copies = [remote(l_src(t), l_v.at[l_slice(t, j)], lsend.at[t], lrecv.at[t], at(y, x, 1 - j)) for t in range(nt)]
    def start_all(copies):
        for copy in copies:
            copy.start()

    def arrive(m, d, fwd=None):
        came(m, d)
        if fwd is not None:
            passes[fwd].start()
        place(m, d)

    items = {
        "g": lambda: start_all(gathers),
        "p0": lambda: (place(0, 0), place(1, 0)),
        "L": lambda: start_all(l_copies),
        "a01": lambda: arrive(0, 1, 1),
        "a13": lambda: arrive(1, ny - 1, 0),
        "a11": lambda: arrive(1, 1),
        "a03": lambda: arrive(0, ny - 1),
        "a02": lambda: arrive(0, 2),
        "a12": lambda: arrive(1, 2),
    }
    for t in range(1, nt):
        items["x%d" % t] = functools.partial(x_first, t)
        items["h%d" % t] = functools.partial(forward_held, t)
        items["fe%d" % t] = functools.partial(forward_passed, t, p_end)
        items["fm%d" % t] = functools.partial(forward_passed, t, p_mid)
    for t in range(nt):
        items["E%d" % t] = functools.partial(ends, t)
        items["M%d" % t] = functools.partial(middles, t)
        items["G%d" % t] = functools.partial(merge, t)
        items["F%d" % t] = lambda t=t: [finish(t, h) for h in range(2)]
    for name in ORDER:
        items[name]()

    for copy in gathers + passes + l_copies:
        copy.wait_send()
    for m in range(2):
        for d in range(ny):
            xt, away, _ = place_copy(m, d)

            @pl.when(xt != x)
            def _():
                away().wait_send()
    for m in range(2, 2 * nt):
        xt, away, _ = x_copy(m)

        @pl.when(xt != x)
        def _():
            away().wait_send()
    for t in range(1, nt):
        for p in range(2):
            for q in range(2):
                @pl.when(is_holder)
                def _():
                    y_copy(t, p, q, s_own, 0, y_outer).wait_send()
                    y_copy(t, p, q, s_own, 1, y_partner).wait_send()

                @pl.when(jnp.logical_not(is_holder))
                def _():
                    y_copy(t, p, q, 1 - s_own, 0, y_next).wait_send()
    for t in range(nt):
        for h in range(2):
            far_copy(t, h).wait_send()
            end_copy(t, 1 - h, h).wait_send()
    for t in range(nt - 1):
        for h in range(2):
            end_copy(t, h, h).wait_send()
    for h in range(2):
        finish(nt - 1, h)
    for h in range(2):
        end_copy(nt - 1, h, h).wait_send()


def solution(mesh):
    ny = mesh.shape["row"]
    nx = mesh.shape["col"] // CORES

    def local_product(lower_loc, rhs_loc):
        rows, width = lower_loc.shape
        cols = rhs_loc.shape[1]
        nt = width // BLOCK
        dma = pltpu.SemaphoreType.DMA
        return pl.pallas_call(
            functools.partial(kernel, ny, nx, nt),
            out_shape=pltpu.VMEM((cols, rows), BF16),
            in_specs=[pl.BlockSpec(memory_space=pl.ANY)] * 2,
            out_specs=pl.BlockSpec(memory_space=pltpu.VMEM),
            scratch_shapes=[
                pltpu.VMEM((rows, CORES * width), BF16),
                pltpu.VMEM((cols, rows), BF16),
                pltpu.VMEM((2 * ny, cols, BLOCK), BF16),
                pltpu.VMEM((nt, 2, 2, 2, cols, BLOCK), BF16),
                pltpu.VMEM((nt, 2, 2, 2, cols, BLOCK), F32),
                pltpu.VMEM((nt, 2, cols, BLOCK), F32),
                pltpu.VMEM((nt, 2, 2, cols, BLOCK), F32),
                dma((nt,)), dma((nt,)), dma((nt,)), dma, dma((6 + 2 * ny,)), dma((2 * ny,)), dma((2 * nt,)),
                dma((nt, 2, 2, 2)), dma((nt, 2, 2, 2)), dma((nt, 6)), dma((nt, 2)), dma((nt, 2, 2)),
            ],
            compiler_params=pltpu.CompilerParams(collective_id=0, has_side_effects=True),
        )(lower_loc, rhs_loc.T).T

    return jax.shard_map(local_product, mesh=mesh, in_specs=(P("row", "col"), P("row", ("batch", "col"))),
                         out_specs=P("row", ("batch", "col")), check_vma=False)
```

```python
import functools

import jax
import jax.numpy as jnp
from jax import lax
from jax.experimental import pallas as pl
from jax.experimental.pallas import tpu as pltpu
from jax.sharding import PartitionSpec as P

ORDER = (
    "g", "p0", "x1", "L", "a01", "a03", "a11", "a13", "x2", "a02", "a12", "h1", "E0", "M0", "h2", "fe1",
    "fm1", "G0", "E1", "fe2", "M1", "fm2", "E2", "M2", "G1", "F0", "G2", "F1",
)
BLOCK = 256
CORES = 2
F32, BF16 = jnp.float32, jnp.bfloat16


def kernel(ny, nx, nt, l_hbm, b_hbm, x_out, l_v, b_v, b_col, b_all, part, far_in, end_in, l_sem, lsend, lrecv, bload, gsend, psem,
           xsend, ysend, fsend, esend, grecv, brecv, far_sem, end_sem):
    cols = b_hbm.shape[0]
    y = lax.axis_index("row")
    c = lax.axis_index("col")
    x, j = c // CORES, c % CORES

    def at(yy, xx, jj=j):
        return {"row": yy, "col": CORES * xx + jj}

    def remote(src, dst, send, recv, dev):
        return pltpu.make_async_remote_copy(src_ref=src, dst_ref=dst, send_sem=send, recv_sem=recv, device_id=dev,
                                            device_id_type=pl.DeviceIdType.MESH)

    def landed(ref, sem):
        pltpu.make_async_copy(ref, ref, sem).wait()

    xr, xl = (x + 1) % nx, (x + nx - 1) % nx
    yu, yd = (y + 1) % ny, (y + ny - 1) % ny
    p_end, p_mid = x % 2, 1 - x % 2

    load_b = pltpu.make_async_copy(b_hbm, b_v, bload)
    load_b.start()

    def l_slice(t, core):
        return (pl.ds(2 * t * BLOCK, (2 * nt - 2 * t) * BLOCK), pl.ds(pl.multiple_of((2 * t + core) * BLOCK, BLOCK), BLOCK))

    def l_src(t):
        return l_hbm.at[pl.ds(2 * t * BLOCK, (2 * nt - 2 * t) * BLOCK), pl.ds(t * BLOCK, BLOCK)]

    load_l = [pltpu.make_async_copy(l_src(t), l_v.at[l_slice(t, j)], l_sem) for t in range(nt)]
    for copy in load_l:
        copy.start()

    barrier = pltpu.get_barrier_semaphore()
    peers = [at(y, x, 1 - j)] + [at(y, (x + d) % nx) for d in range(1, nx)] + [at(yu, x), at(yd, x)]
    for dev in peers:
        pl.semaphore_signal(barrier, inc=1, device_id=dev, device_id_type=pl.DeviceIdType.MESH)
    load_b.wait()
    pl.semaphore_wait(barrier, len(peers))

    def b_block(m):
        return b_v.at[:, pl.ds(m * BLOCK, BLOCK)]

    s_own = y % 2
    chunk_p, chunk_q = x % 2, x // 2

    def gather_copy(m, yy, i):
        k = ny * m + y
        return remote(b_block(m), b_col.at[k], gsend, grecv.at[k], at(yy, x))

    def pass_copy(m, y_from, y_to, i):
        r = b_col.at[ny * m + y_from]
        return remote(r, r, gsend, grecv.at[ny * m + y_from], at(y_to, x))

    gathers = [gather_copy(0, yu, 0), gather_copy(0, yd, 1), gather_copy(1, yu, 2), gather_copy(1, yd, 3)]
    passes = [pass_copy(1, yd, yu, 4), pass_copy(0, yu, yd, 5)]

    def place_copy(m, d):
        yy = (y + d) % ny
        src = b_col.at[ny * m + yy] if d else b_block(m)
        dst, sem = b_all.at[0, chunk_p, yy % 2, chunk_q], brecv.at[0, chunk_p, yy % 2, chunk_q]
        xt = yy // 2 + 2 * m
        return xt, (lambda: remote(src, dst, psem, sem, at(y, xt))), (lambda: pltpu.make_async_copy(src, dst, sem))

    def came(m, d):
        k = ny * m + (y + d) % ny
        landed(b_col.at[k], grecv.at[k])

    def place(m, d):
        xt, away, here = place_copy(m, d)

        @pl.when(xt != x)
        def _():
            away().start()

        @pl.when(xt == x)
        def _():
            here().start()

    def x_copy(m):
        xt = y // 2 + 2 * (m % 2)
        dst, sem = b_all.at[m // 2, chunk_p, s_own, chunk_q], brecv.at[m // 2, chunk_p, s_own, chunk_q]
        return xt, (lambda: remote(b_block(m), dst, xsend, sem, at(y, xt))), (lambda: pltpu.make_async_copy(b_block(m), dst, sem))

    def x_first(t):
        for m in (2 * t, 2 * t + 1):
            xt, away, here = x_copy(m)

            @pl.when(xt != x)
            def _():
                away().start()

            @pl.when(xt == x)
            def _():
                here().start()

    is_holder = (y // 2) == (x % 2)
    hx = 2 * (x % 2)
    y_partner = hx + 1 - s_own
    y_outer = (y + ny + 2 * s_own - 1) % ny
    y_next = (y + ny + 1 - 2 * s_own) % ny
    held = is_holder.astype(jnp.int32)
    s_first = held * s_own + (1 - held) * (1 - s_own)

    def y_copy(t, p, s, q, yy):
        r = b_all.at[t, p, s, q]
        return remote(r, r, ysend, brecv.at[t, p, s, q], at(yy, x))

    def b_came(t, p, s, q):
        landed(b_all.at[t, p, s, q], brecv.at[t, p, s, q])

    def forward_held(t):
        @pl.when(is_holder)
        def _():
            for p in (p_end, p_mid):
                for q in range(2):
                    b_came(t, p, s_own, q)
                    y_copy(t, p, s_own, q, y_outer).start()
                    y_copy(t, p, s_own, q, y_partner).start()

    def forward_passed(t, p):
        @pl.when(jnp.logical_not(is_holder))
        def _():
            for q in range(2):
                b_came(t, p, 1 - s_own, q)
                y_copy(t, p, 1 - s_own, q, y_next).start()

    def compute(t, role):
        p = (p_end, p_mid)[role]
        if t == 0:
            for s in range(2):
                @pl.when(CORES * x + s <= y + ny)
                def _():
                    for q in range(2):
                        b_came(t, p, s, q)
        else:
            for q in range(2):
                b_came(t, p, 1 - s_first, q)
        if t == 1:
            for s in range(2):
                @pl.when(CORES * x + s > y + ny)
                def _():
                    for q in range(2):
                        b_came(0, p, s, q)
        if role == 0 and t == 0:
            l_all = l_v.at[pl.ds(0, (nt + 1) * BLOCK // 2), :]
            landed(l_all, l_sem)
            landed(l_all, lrecv)
        for h in range(2):
            m = 2 * t + h
            if t == 0:
                part[t, role, :, h] = jnp.zeros((2, cols, BLOCK), F32)
                for s in range(2):
                    @pl.when(CORES * x + s <= y + ny * h)
                    def _():
                        lhs = b_all[0, p, s].reshape(2 * cols, BLOCK)
                        rhs = l_v[m * BLOCK:(m + 1) * BLOCK, s * BLOCK:(s + 1) * BLOCK]
                        acc = lax.dot_general(lhs, rhs, (((1,), (1,)), ((), ())), preferred_element_type=F32)
                        part[t, role, :, h] += acc.reshape(2, cols, BLOCK)
                continue
            acc = jnp.zeros((2 * cols, BLOCK), F32)
            for u in range(t + 1):
                for s in range(2):
                    lhs = b_all[u, p, s].reshape(2 * cols, BLOCK)
                    rhs = l_v[m * BLOCK:(m + 1) * BLOCK, (2 * u + s) * BLOCK:(2 * u + s + 1) * BLOCK]
                    acc += lax.dot_general(lhs, rhs, (((1,), (1,)), ((), ())), preferred_element_type=F32)
            part[t, role, :, h] = acc.reshape(2, cols, BLOCK)

    q_own = x // 2

    def far_copy(t, h):
        return remote(part.at[t, 0, 1 - q_own, h], far_in.at[t, h], fsend, far_sem.at[t, h], at(y, xl if h else xr))

    def end_copy(t, side, h):
        xx = xl if side else xr
        return remote(part.at[t, 1, xx // 2, h], end_in.at[t, h, side], esend, end_sem.at[t, h], at(y, xx))

    def ends(t):
        compute(t, 0)
        far_copy(t, 0).start()
        far_copy(t, 1).start()

    def middles(t):
        compute(t, 1)
        end_copy(t, 0, 1).start()
        end_copy(t, 1, 0).start()

    def merge(t):
        for h, xx in ((0, xr), (1, xl)):
            landed(far_in.at[t, h], far_sem.at[t, h])
            part[t, 1, xx // 2, h] += far_in[t, h]
            end_copy(t, h, h).start()

    def finish(t, h):
        landed(end_in.at[t, h], end_sem.at[t, h])
        m = 2 * t + h
        x_out[:, m * BLOCK:(m + 1) * BLOCK] = (part[t, 0, q_own, h] + (end_in[t, h, 0] + end_in[t, h, 1])).astype(BF16)

    l_copies = [remote(l_src(t), l_v.at[l_slice(t, j)], lsend, lrecv, at(y, x, 1 - j)) for t in range(nt)]
    def start_all(copies):
        for copy in copies:
            copy.start()

    def arrive(m, d, fwd=None):
        came(m, d)
        if fwd is not None:
            passes[fwd].start()
        place(m, d)

    items = {
        "g": lambda: start_all(gathers),
        "p0": lambda: (place(0, 0), place(1, 0)),
        "L": lambda: start_all(l_copies),
        "a01": lambda: arrive(0, 1, 1),
        "a13": lambda: arrive(1, ny - 1, 0),
        "a11": lambda: arrive(1, 1),
        "a03": lambda: arrive(0, ny - 1),
        "a02": lambda: arrive(0, 2),
        "a12": lambda: arrive(1, 2),
    }
    for t in range(1, nt):
        items["x%d" % t] = functools.partial(x_first, t)
        items["h%d" % t] = functools.partial(forward_held, t)
        items["fe%d" % t] = functools.partial(forward_passed, t, p_end)
        items["fm%d" % t] = functools.partial(forward_passed, t, p_mid)
    for t in range(nt):
        items["E%d" % t] = functools.partial(ends, t)
        items["M%d" % t] = functools.partial(middles, t)
        items["G%d" % t] = functools.partial(merge, t)
        items["F%d" % t] = lambda t=t: [finish(t, h) for h in range(2)]
    for name in ORDER:
        items[name]()

    landed(l_v.at[pl.ds(0, (nt + 1) * BLOCK // 2), :], lsend)
    landed(b_v, gsend)
    landed(b_col.at[pl.ds(0, 2 * (ny - 1))], psem)

    @pl.when(y // 2 == x % 2)
    def _():
        landed(b_v.at[:, pl.ds(0, (nt - 1) * BLOCK)], xsend)
        landed(b_all.at[pl.ds(0, nt - 1)], ysend)

    @pl.when(y // 2 != x % 2)
    def _():
        landed(b_v.at[:, pl.ds(0, 2 * (nt - 1) * BLOCK)], xsend)
        landed(b_all.at[pl.ds(0, nt - 1), :, 0], ysend)

    landed(far_in, fsend)
    for h in range(2):
        finish(nt - 1, h)
    landed(end_in, esend)


def solution(mesh):
    ny = mesh.shape["row"]
    nx = mesh.shape["col"] // CORES

    def local_product(lower_loc, rhs_loc):
        rows, width = lower_loc.shape
        cols = rhs_loc.shape[1]
        nt = width // BLOCK
        dma = pltpu.SemaphoreType.DMA
        return pl.pallas_call(
            functools.partial(kernel, ny, nx, nt),
            out_shape=pltpu.VMEM((cols, rows), BF16),
            in_specs=[pl.BlockSpec(memory_space=pl.ANY)] * 2,
            out_specs=pl.BlockSpec(memory_space=pltpu.VMEM),
            scratch_shapes=[
                pltpu.VMEM((rows, CORES * width), BF16),
                pltpu.VMEM((cols, rows), BF16),
                pltpu.VMEM((2 * ny, cols, BLOCK), BF16),
                pltpu.VMEM((nt, 2, 2, 2, cols, BLOCK), BF16),
                pltpu.VMEM((nt, 2, 2, 2, cols, BLOCK), F32),
                pltpu.VMEM((nt, 2, cols, BLOCK), F32),
                pltpu.VMEM((nt, 2, 2, cols, BLOCK), F32),
                *[dma] * 10, dma((2 * ny,)), dma((nt, 2, 2, 2)), dma((nt, 2)), dma((nt, 2)),
            ],
            compiler_params=pltpu.CompilerParams(collective_id=0, has_side_effects=True),
        )(lower_loc, rhs_loc.T).T

    return jax.shard_map(local_product, mesh=mesh, in_specs=(P("row", "col"), P("row", ("batch", "col"))),
                         out_specs=P("row", ("batch", "col")), check_vma=False)
```

```python
import functools

import jax
import jax.numpy as jnp
from jax import lax
from jax.experimental import pallas as pl
from jax.experimental.pallas import tpu as pltpu
from jax.sharding import PartitionSpec as P

ORDER = (
    "g", "x1", "L", "p0", "a01", "a03", "a13", "a11", "x2", "a02", "a12", "he1", "E0", "hm1", "M0", "he2",
    "fe1", "hm2", "fm1", "Ga0", "Gb0", "E1", "fe2", "M1", "fm2", "E2", "Ga1", "Gb1", "M2", "F0", "Ga2",
    "Gb2", "F1",
)
BLOCK = 256
CORES = 2
F32, BF16 = jnp.float32, jnp.bfloat16


def kernel(ny, nx, nt, l_hbm, b_hbm, x_out, l_v, b_v, b_col, b_all, part, far_in, end_in, l_sem, lsend, lrecv, bload, gsend, psem,
           xsend, ysend, fsend, esend, grecv, brecv, far_sem, end_sem):
    cols = b_hbm.shape[0]
    y = lax.axis_index("row")
    c = lax.axis_index("col")
    x, j = c // CORES, c % CORES

    def at(yy, xx, jj=j):
        return {"row": yy, "col": CORES * xx + jj}

    def remote(src, dst, send, recv, dev):
        return pltpu.make_async_remote_copy(src_ref=src, dst_ref=dst, send_sem=send, recv_sem=recv, device_id=dev,
                                            device_id_type=pl.DeviceIdType.MESH)

    def landed(ref, sem):
        pltpu.make_async_copy(ref, ref, sem).wait()

    xr, xl = (x + 1) % nx, (x + nx - 1) % nx
    yu, yd = (y + 1) % ny, (y + ny - 1) % ny
    p_end, p_mid = x % 2, 1 - x % 2

    load_b = pltpu.make_async_copy(b_hbm, b_v, bload)
    load_b.start()

    def l_slice(t, core):
        return (pl.ds(2 * t * BLOCK, (2 * nt - 2 * t) * BLOCK), pl.ds(pl.multiple_of((2 * t + core) * BLOCK, BLOCK), BLOCK))

    def l_src(t):
        return l_hbm.at[pl.ds(2 * t * BLOCK, (2 * nt - 2 * t) * BLOCK), pl.ds(t * BLOCK, BLOCK)]

    load_l = [pltpu.make_async_copy(l_src(t), l_v.at[l_slice(t, j)], l_sem) for t in range(nt)]
    for copy in load_l:
        copy.start()

    barrier = pltpu.get_barrier_semaphore()
    peers = [at(y, x, 1 - j)] + [at(y, (x + d) % nx) for d in range(1, nx)] + [at(yu, x), at(yd, x)]
    for dev in peers:
        pl.semaphore_signal(barrier, inc=1, device_id=dev, device_id_type=pl.DeviceIdType.MESH)
    load_b.wait()
    pl.semaphore_wait(barrier, len(peers))

    def b_block(m):
        return b_v.at[:, pl.ds(m * BLOCK, BLOCK)]

    s_own = y % 2
    chunk_p, chunk_q = x % 2, x // 2

    def gather_copy(m, yy, i):
        k = ny * m + y
        return remote(b_block(m), b_col.at[k], gsend, grecv.at[k], at(yy, x))

    def pass_copy(m, y_from, y_to, i):
        r = b_col.at[ny * m + y_from]
        return remote(r, r, gsend, grecv.at[ny * m + y_from], at(y_to, x))

    gathers = [gather_copy(0, yu, 0), gather_copy(0, yd, 1), gather_copy(1, yu, 2), gather_copy(1, yd, 3)]
    passes = [pass_copy(1, yd, yu, 4), pass_copy(0, yu, yd, 5)]

    def place_copy(m, d):
        yy = (y + d) % ny
        src = b_col.at[ny * m + yy] if d else b_block(m)
        dst, sem = b_all.at[0, chunk_p, yy % 2, chunk_q], brecv.at[0, chunk_p, yy % 2, chunk_q]
        xt = yy // 2 + 2 * m
        return xt, (lambda: remote(src, dst, psem, sem, at(y, xt))), (lambda: pltpu.make_async_copy(src, dst, sem))

    def came(m, d):
        k = ny * m + (y + d) % ny
        landed(b_col.at[k], grecv.at[k])

    def place(m, d):
        xt, away, here = place_copy(m, d)

        @pl.when(xt != x)
        def _():
            away().start()

        @pl.when(xt == x)
        def _():
            here().start()

    def x_copy(m):
        xt = y // 2 + 2 * (m % 2)
        dst, sem = b_all.at[m // 2, chunk_p, s_own, chunk_q], brecv.at[m // 2, chunk_p, s_own, chunk_q]
        return xt, (lambda: remote(b_block(m), dst, xsend, sem, at(y, xt))), (lambda: pltpu.make_async_copy(b_block(m), dst, sem))

    def x_first(t):
        for m in (2 * t, 2 * t + 1):
            xt, away, here = x_copy(m)

            @pl.when(xt != x)
            def _():
                away().start()

            @pl.when(xt == x)
            def _():
                here().start()

    is_holder = (y // 2) == (x % 2)
    hx = 2 * (x % 2)
    y_partner = hx + 1 - s_own
    y_outer = (y + ny + 2 * s_own - 1) % ny
    y_next = (y + ny + 1 - 2 * s_own) % ny
    held = is_holder.astype(jnp.int32)
    s_first = held * s_own + (1 - held) * (1 - s_own)

    def y_copy(t, p, s, q, yy):
        r = b_all.at[t, p, s, q]
        return remote(r, r, ysend, brecv.at[t, p, s, q], at(yy, x))

    def b_came(t, p, s, q):
        landed(b_all.at[t, p, s, q], brecv.at[t, p, s, q])

    def forward_held(t, p):
        @pl.when(is_holder)
        def _():
            for q in range(2):
                b_came(t, p, s_own, q)
                y_copy(t, p, s_own, q, y_outer).start()
                y_copy(t, p, s_own, q, y_partner).start()

    def forward_passed(t, p):
        @pl.when(jnp.logical_not(is_holder))
        def _():
            for q in range(2):
                b_came(t, p, 1 - s_own, q)
                y_copy(t, p, 1 - s_own, q, y_next).start()

    def product(p, u, s, m):
        lhs = b_all[u, p, s].reshape(2 * cols, BLOCK)
        rhs = l_v[m * BLOCK:(m + 1) * BLOCK, pl.ds(pl.multiple_of((2 * u + s) * BLOCK, BLOCK), BLOCK)]
        return lax.dot_general(lhs, rhs, (((1,), (1,)), ((), ())), preferred_element_type=F32).reshape(2, cols, BLOCK)

    def await_first(p):
        for s in range(2):
            @pl.when(CORES * x + s <= y + ny)
            def _():
                for q in range(2):
                    b_came(0, p, s, q)

    def await_rest(p):
        for s in range(2):
            @pl.when(CORES * x + s > y + ny)
            def _():
                for q in range(2):
                    b_came(0, p, s, q)

    def compute(t, role, sends):
        p = (p_end, p_mid)[role]
        s_last = 1 - s_first
        if t == 0:
            await_first(p)
        if t == 1:
            await_rest(p)
        if role == 0 and t == 0:
            l_all = l_v.at[pl.ds(0, (nt + 1) * BLOCK // 2), :]
            landed(l_all, l_sem)
            landed(l_all, lrecv)
        if t:
            for h in range(2):
                acc = product(p, t, s_first, 2 * t + h)
                for u in range(t):
                    for s in range(2):
                        acc += product(p, u, s, 2 * t + h)
                part[t, role, :, h] = acc
            for q in range(2):
                b_came(t, p, s_last, q)
        for h in range(2):
            m = 2 * t + h
            if t:
                part[t, role, :, h] += product(p, t, s_last, m)
            else:
                part[t, role, :, h] = jnp.zeros((2, cols, BLOCK), F32)
                for s in range(2):
                    @pl.when(CORES * x + s <= y + ny * h)
                    def _():
                        part[t, role, :, h] += product(p, 0, s, m)
            sends[h].start()

    q_own = x // 2

    def far_copy(t, h):
        return remote(part.at[t, 0, 1 - q_own, h], far_in.at[t, h], fsend, far_sem.at[t, h], at(y, xl if h else xr))

    def end_copy(t, side, h):
        xx = xl if side else xr
        return remote(part.at[t, 1, xx // 2, h], end_in.at[t, h, side], esend, end_sem.at[t, h], at(y, xx))

    def ends(t):
        compute(t, 0, [far_copy(t, 0), far_copy(t, 1)])

    def middles(t):
        compute(t, 1, [end_copy(t, 1, 0), end_copy(t, 0, 1)])

    def merge(t, h):
        xx = xl if h else xr
        landed(far_in.at[t, h], far_sem.at[t, h])
        part[t, 1, xx // 2, h] += far_in[t, h]
        end_copy(t, h, h).start()

    def finish(t, h):
        landed(end_in.at[t, h], end_sem.at[t, h])
        m = 2 * t + h
        x_out[:, m * BLOCK:(m + 1) * BLOCK] = (part[t, 0, q_own, h] + (end_in[t, h, 0] + end_in[t, h, 1])).astype(BF16)

    l_copies = [remote(l_src(t), l_v.at[l_slice(t, j)], lsend, lrecv, at(y, x, 1 - j)) for t in range(nt)]
    def start_all(copies):
        for copy in copies:
            copy.start()

    def arrive(m, d, fwd=None):
        came(m, d)
        if fwd is not None:
            passes[fwd].start()
        place(m, d)

    items = {
        "g": lambda: start_all(gathers),
        "p0": lambda: (place(0, 0), place(1, 0)),
        "L": lambda: start_all(l_copies),
        "a01": lambda: arrive(0, 1, 1),
        "a13": lambda: arrive(1, ny - 1, 0),
        "a11": lambda: arrive(1, 1),
        "a03": lambda: arrive(0, ny - 1),
        "a02": lambda: arrive(0, 2),
        "a12": lambda: arrive(1, 2),
    }
    for t in range(1, nt):
        items["x%d" % t] = functools.partial(x_first, t)
        items["he%d" % t] = functools.partial(forward_held, t, p_end)
        items["hm%d" % t] = functools.partial(forward_held, t, p_mid)
        items["fe%d" % t] = functools.partial(forward_passed, t, p_end)
        items["fm%d" % t] = functools.partial(forward_passed, t, p_mid)
    for t in range(nt):
        items["E%d" % t] = functools.partial(ends, t)
        items["M%d" % t] = functools.partial(middles, t)
        items["Ga%d" % t] = functools.partial(merge, t, 0)
        items["Gb%d" % t] = functools.partial(merge, t, 1)
        items["F%d" % t] = lambda t=t: [finish(t, h) for h in range(2)]
    for name in ORDER:
        items[name]()

    landed(l_v.at[pl.ds(0, (nt + 1) * BLOCK // 2), :], lsend)
    landed(b_v, gsend)
    landed(b_col.at[pl.ds(0, 2 * (ny - 1))], psem)

    @pl.when(y // 2 == x % 2)
    def _():
        landed(b_v.at[:, pl.ds(0, (nt - 1) * BLOCK)], xsend)
        landed(b_all.at[pl.ds(0, nt - 1)], ysend)

    @pl.when(y // 2 != x % 2)
    def _():
        landed(b_v.at[:, pl.ds(0, 2 * (nt - 1) * BLOCK)], xsend)
        landed(b_all.at[pl.ds(0, nt - 1), :, 0], ysend)

    landed(far_in, fsend)
    for h in range(2):
        finish(nt - 1, h)
    landed(end_in, esend)


def solution(mesh):
    ny = mesh.shape["row"]
    nx = mesh.shape["col"] // CORES

    def local_product(lower_loc, rhs_loc):
        rows, width = lower_loc.shape
        cols = rhs_loc.shape[1]
        nt = width // BLOCK
        dma = pltpu.SemaphoreType.DMA
        return pl.pallas_call(
            functools.partial(kernel, ny, nx, nt),
            out_shape=pltpu.VMEM((cols, rows), BF16),
            in_specs=[pl.BlockSpec(memory_space=pl.ANY)] * 2,
            out_specs=pl.BlockSpec(memory_space=pltpu.VMEM),
            scratch_shapes=[
                pltpu.VMEM((rows, CORES * width), BF16),
                pltpu.VMEM((cols, rows), BF16),
                pltpu.VMEM((2 * ny, cols, BLOCK), BF16),
                pltpu.VMEM((nt, 2, 2, 2, cols, BLOCK), BF16),
                pltpu.VMEM((nt, 2, 2, 2, cols, BLOCK), F32),
                pltpu.VMEM((nt, 2, cols, BLOCK), F32),
                pltpu.VMEM((nt, 2, 2, cols, BLOCK), F32),
                *[dma] * 10, dma((2 * ny,)), dma((nt, 2, 2, 2)), dma((nt, 2)), dma((nt, 2)),
            ],
            compiler_params=pltpu.CompilerParams(collective_id=0, has_side_effects=True),
        )(lower_loc, rhs_loc.T).T

    return jax.shard_map(local_product, mesh=mesh, in_specs=(P("row", "col"), P("row", ("batch", "col"))),
                         out_specs=P("row", ("batch", "col")), check_vma=False)
```

```python
import functools

import jax
import jax.numpy as jnp
from jax import lax
from jax.experimental import pallas as pl
from jax.experimental.pallas import tpu as pltpu
from jax.sharding import PartitionSpec as P

ORDER = (
    "g", "x1", "L", "p0", "a01", "a03", "a13", "a11", "x2", "a02", "a12", "he1", "E0", "hm1", "M0", "he2",
    "fe1", "hm2", "fm1", "Ga0", "Gb0", "E1", "fe2", "M1", "fm2", "E2", "Ga1", "Gb1", "M2", "F0", "Ga2",
    "Gb2", "F1",
)
BLOCK = 256
CORES = 2
F32, BF16 = jnp.float32, jnp.bfloat16


def kernel(ny, nx, nt, l_hbm, b_hbm, x_out, l_v, b_v, b_col, b_all, part, far_in, end_in, l_sem, lsend, lrecv, bload, gsend,
           xsend, ysend, fsend, esend, grecv, bfirst, brecv, far_sem, end_sem):
    cols = b_hbm.shape[0]
    y = lax.axis_index("row")
    c = lax.axis_index("col")
    x, j = c // CORES, c % CORES

    def at(yy, xx, jj=j):
        return {"row": yy, "col": CORES * xx + jj}

    def remote(src, dst, send, recv, dev):
        return pltpu.make_async_remote_copy(src_ref=src, dst_ref=dst, send_sem=send, recv_sem=recv, device_id=dev,
                                            device_id_type=pl.DeviceIdType.MESH)

    def landed(ref, sem):
        pltpu.make_async_copy(ref, ref, sem).wait()

    xr, xl = (x + 1) % nx, (x + nx - 1) % nx
    yu, yd = (y + 1) % ny, (y + ny - 1) % ny
    p_end, p_mid = x % 2, 1 - x % 2

    load_b = pltpu.make_async_copy(b_hbm, b_v, bload)
    load_b.start()

    def l_slice(t, core):
        return (pl.ds(2 * t * BLOCK, (2 * nt - 2 * t) * BLOCK), pl.ds(pl.multiple_of((2 * t + core) * BLOCK, BLOCK), BLOCK))

    def l_src(t):
        return l_hbm.at[pl.ds(2 * t * BLOCK, (2 * nt - 2 * t) * BLOCK), pl.ds(t * BLOCK, BLOCK)]

    load_l = [pltpu.make_async_copy(l_src(t), l_v.at[l_slice(t, j)], l_sem) for t in range(nt)]
    for copy in load_l:
        copy.start()

    barrier = pltpu.get_barrier_semaphore()
    peers = [at(y, x, 1 - j)] + [at(y, (x + d) % nx) for d in range(1, nx)] + [at(yu, x), at(yd, x)]
    for dev in peers:
        pl.semaphore_signal(barrier, inc=1, device_id=dev, device_id_type=pl.DeviceIdType.MESH)
    load_b.wait()
    pl.semaphore_wait(barrier, len(peers))

    def b_block(m):
        return b_v.at[:, pl.ds(m * BLOCK, BLOCK)]

    s_own = y % 2
    chunk_p, chunk_q = x % 2, x // 2

    def gather_copy(m, yy, i):
        k = ny * m + y
        return remote(b_block(m), b_col.at[k], gsend, grecv.at[k], at(yy, x))

    def pass_copy(m, y_from, y_to, i):
        r = b_col.at[ny * m + y_from]
        return remote(r, r, gsend, grecv.at[ny * m + y_from], at(y_to, x))

    gathers = [gather_copy(0, yu, 0), gather_copy(0, yd, 1), gather_copy(1, yu, 2), gather_copy(1, yd, 3)]
    passes = [pass_copy(1, yd, yu, 4), pass_copy(0, yu, yd, 5)]

    def place_copy(m, d):
        yy = (y + d) % ny
        src = b_col.at[ny * m + yy] if d else b_block(m)
        dst, sem = b_all.at[0, chunk_p, yy % 2, chunk_q], bfirst.at[chunk_p, yy % 2]
        xt = yy // 2 + 2 * m
        return xt, (lambda: remote(src, dst, gsend, sem, at(y, xt))), (lambda: pltpu.make_async_copy(src, dst, sem))

    def came(m, d):
        k = ny * m + (y + d) % ny
        landed(b_col.at[k], grecv.at[k])

    def place(m, d):
        xt, away, here = place_copy(m, d)

        @pl.when(xt != x)
        def _():
            away().start()

        @pl.when(xt == x)
        def _():
            here().start()

    def x_copy(m):
        xt = y // 2 + 2 * (m % 2)
        dst, sem = b_all.at[m // 2, chunk_p, s_own, chunk_q], brecv.at[m // 2 - 1, chunk_p, s_own, chunk_q]
        return xt, (lambda: remote(b_block(m), dst, xsend, sem, at(y, xt))), (lambda: pltpu.make_async_copy(b_block(m), dst, sem))

    def x_first(t):
        for m in (2 * t, 2 * t + 1):
            xt, away, here = x_copy(m)

            @pl.when(xt != x)
            def _():
                away().start()

            @pl.when(xt == x)
            def _():
                here().start()

    is_holder = (y // 2) == (x % 2)
    hx = 2 * (x % 2)
    y_partner = hx + 1 - s_own
    y_outer = (y + ny + 2 * s_own - 1) % ny
    y_next = (y + ny + 1 - 2 * s_own) % ny
    held = is_holder.astype(jnp.int32)
    s_first = held * s_own + (1 - held) * (1 - s_own)

    def y_copy(t, p, s, q, yy):
        r = b_all.at[t, p, s, q]
        return remote(r, r, ysend, brecv.at[t - 1, p, s, q], at(yy, x))

    def b_came(t, p, s, q):
        landed(b_all.at[t, p, s, q], brecv.at[t - 1, p, s, q])

    def forward_held(t, p):
        @pl.when(is_holder)
        def _():
            for q in range(2):
                b_came(t, p, s_own, q)
                y_copy(t, p, s_own, q, y_outer).start()
                y_copy(t, p, s_own, q, y_partner).start()

    def forward_passed(t, p):
        @pl.when(jnp.logical_not(is_holder))
        def _():
            for q in range(2):
                b_came(t, p, 1 - s_own, q)
                y_copy(t, p, 1 - s_own, q, y_next).start()

    def product(p, u, s, m):
        lhs = b_all[u, p, s].reshape(2 * cols, BLOCK)
        rhs = l_v[m * BLOCK:(m + 1) * BLOCK, pl.ds(pl.multiple_of((2 * u + s) * BLOCK, BLOCK), BLOCK)]
        return lax.dot_general(lhs, rhs, (((1,), (1,)), ((), ())), preferred_element_type=F32).reshape(2, cols, BLOCK)

    def await_first(p):
        for s in range(2):
            @pl.when(CORES * x + s <= y + ny)
            def _():
                landed(b_all.at[0, p, s], bfirst.at[p, s])

    def await_rest(p):
        for s in range(2):
            @pl.when(CORES * x + s > y + ny)
            def _():
                landed(b_all.at[0, p, s], bfirst.at[p, s])

    def compute(t, role, sends):
        p = (p_end, p_mid)[role]
        s_last = 1 - s_first
        if t == 0:
            await_first(p)
        if t == 1:
            await_rest(p)
        if role == 0 and t == 0:
            l_all = l_v.at[pl.ds(0, (nt + 1) * BLOCK // 2), :]
            landed(l_all, l_sem)
            landed(l_all, lrecv)
        if t:
            for h in range(2):
                acc = product(p, t, s_first, 2 * t + h)
                for u in range(t):
                    for s in range(2):
                        acc += product(p, u, s, 2 * t + h)
                part[t, role, :, h] = acc
            for q in range(2):
                b_came(t, p, s_last, q)
        for h in range(2):
            m = 2 * t + h
            if t:
                part[t, role, :, h] += product(p, t, s_last, m)
            else:
                part[t, role, :, h] = jnp.zeros((2, cols, BLOCK), F32)
                for s in range(2):
                    @pl.when(CORES * x + s <= y + ny * h)
                    def _():
                        part[t, role, :, h] += product(p, 0, s, m)
            sends[h].start()

    q_own = x // 2

    def far_copy(t, h):
        return remote(part.at[t, 0, 1 - q_own, h], far_in.at[t, h], fsend, far_sem.at[t, h], at(y, xl if h else xr))

    def end_copy(t, side, h):
        xx = xl if side else xr
        return remote(part.at[t, 1, xx // 2, h], end_in.at[t, h, side], esend, end_sem.at[t, h], at(y, xx))

    def ends(t):
        compute(t, 0, [far_copy(t, 0), far_copy(t, 1)])

    def middles(t):
        compute(t, 1, [end_copy(t, 1, 0), end_copy(t, 0, 1)])

    def merge(t, h):
        xx = xl if h else xr
        landed(far_in.at[t, h], far_sem.at[t, h])
        part[t, 1, xx // 2, h] += far_in[t, h]
        end_copy(t, h, h).start()

    def finish(t, h):
        landed(end_in.at[t, h], end_sem.at[t, h])
        m = 2 * t + h
        x_out[:, m * BLOCK:(m + 1) * BLOCK] = (part[t, 0, q_own, h] + (end_in[t, h, 0] + end_in[t, h, 1])).astype(BF16)

    l_copies = [remote(l_src(t), l_v.at[l_slice(t, j)], lsend, lrecv, at(y, x, 1 - j)) for t in range(nt)]
    def start_all(copies):
        for copy in copies:
            copy.start()

    def arrive(m, d, fwd=None):
        came(m, d)
        if fwd is not None:
            passes[fwd].start()
        place(m, d)

    items = {
        "g": lambda: start_all(gathers),
        "p0": lambda: (place(0, 0), place(1, 0)),
        "L": lambda: start_all(l_copies),
        "a01": lambda: arrive(0, 1, 1),
        "a13": lambda: arrive(1, ny - 1, 0),
        "a11": lambda: arrive(1, 1),
        "a03": lambda: arrive(0, ny - 1),
        "a02": lambda: arrive(0, 2),
        "a12": lambda: arrive(1, 2),
    }
    for t in range(1, nt):
        items["x%d" % t] = functools.partial(x_first, t)
        items["he%d" % t] = functools.partial(forward_held, t, p_end)
        items["hm%d" % t] = functools.partial(forward_held, t, p_mid)
        items["fe%d" % t] = functools.partial(forward_passed, t, p_end)
        items["fm%d" % t] = functools.partial(forward_passed, t, p_mid)
    for t in range(nt):
        items["E%d" % t] = functools.partial(ends, t)
        items["M%d" % t] = functools.partial(middles, t)
        items["Ga%d" % t] = functools.partial(merge, t, 0)
        items["Gb%d" % t] = functools.partial(merge, t, 1)
        items["F%d" % t] = lambda t=t: [finish(t, h) for h in range(2)]
    for name in ORDER:
        items[name]()

    landed(l_v.at[pl.ds(0, (nt + 1) * BLOCK // 2), :], lsend)
    landed(b_all.at[:, :, 0], gsend)

    @pl.when(y // 2 == x % 2)
    def _():
        landed(b_v.at[:, pl.ds(0, (nt - 1) * BLOCK)], xsend)
        landed(b_all.at[pl.ds(0, nt - 1)], ysend)

    @pl.when(y // 2 != x % 2)
    def _():
        landed(b_v.at[:, pl.ds(0, 2 * (nt - 1) * BLOCK)], xsend)
        landed(b_all.at[pl.ds(0, nt - 1), :, 0], ysend)

    landed(far_in, fsend)
    for h in range(2):
        finish(nt - 1, h)
    landed(end_in, esend)


def solution(mesh):
    ny = mesh.shape["row"]
    nx = mesh.shape["col"] // CORES

    def local_product(lower_loc, rhs_loc):
        rows, width = lower_loc.shape
        cols = rhs_loc.shape[1]
        nt = width // BLOCK
        dma = pltpu.SemaphoreType.DMA
        return pl.pallas_call(
            functools.partial(kernel, ny, nx, nt),
            out_shape=pltpu.VMEM((cols, rows), BF16),
            in_specs=[pl.BlockSpec(memory_space=pl.ANY)] * 2,
            out_specs=pl.BlockSpec(memory_space=pltpu.VMEM),
            scratch_shapes=[
                pltpu.VMEM((rows, CORES * width), BF16),
                pltpu.VMEM((cols, rows), BF16),
                pltpu.VMEM((2 * ny, cols, BLOCK), BF16),
                pltpu.VMEM((nt, 2, 2, 2, cols, BLOCK), BF16),
                pltpu.VMEM((nt, 2, 2, 2, cols, BLOCK), F32),
                pltpu.VMEM((nt, 2, cols, BLOCK), F32),
                pltpu.VMEM((nt, 2, 2, cols, BLOCK), F32),
                *[dma] * 9, dma((2 * ny,)), dma((2, 2)), dma((nt - 1, 2, 2, 2)), dma((nt, 2)), dma((nt, 2)),
            ],
            compiler_params=pltpu.CompilerParams(collective_id=0, has_side_effects=True),
        )(lower_loc, rhs_loc.T).T

    return jax.shard_map(local_product, mesh=mesh, in_specs=(P("row", "col"), P("row", ("batch", "col"))),
                         out_specs=P("row", ("batch", "col")), check_vma=False)
```

```python
import functools

import jax
import jax.numpy as jnp
from jax import lax
from jax.experimental import pallas as pl
from jax.experimental.pallas import tpu as pltpu
from jax.sharding import PartitionSpec as P

ORDER = (
    "g", "x1", "L", "p0", "a01", "a03", "a13", "a11", "x2", "a02", "a12", "he1", "E0", "hm1", "M0", "he2",
    "fe1", "hm2", "fm1", "Ga0", "Gb0", "E1", "fe2", "M1", "fm2", "E2", "Ga1", "Gb1", "M2", "F0", "Ga2",
    "Gb2", "F1",
)
BLOCK = 256
CORES = 2
F32, BF16 = jnp.float32, jnp.bfloat16


def kernel(ny, nx, nt, l_hbm, b_hbm, x_out, l_v, b_v, b_col, b_all, part, far_in, end_in, l_sem, lsend, bload, gsend,
           xsend, ysend, fsend, esend, grecv, bfirst, brecv, far_sem, end_sem):
    cols = b_hbm.shape[0]
    y = lax.axis_index("row")
    c = lax.axis_index("col")
    x, j = c // CORES, c % CORES

    def at(yy, xx, jj=j):
        return {"row": yy, "col": CORES * xx + jj}

    def remote(src, dst, send, recv, dev):
        return pltpu.make_async_remote_copy(src_ref=src, dst_ref=dst, send_sem=send, recv_sem=recv, device_id=dev,
                                            device_id_type=pl.DeviceIdType.MESH)

    def landed(ref, sem):
        pltpu.make_async_copy(ref, ref, sem).wait()

    xr, xl = (x + 1) % nx, (x + nx - 1) % nx
    yu, yd = (y + 1) % ny, (y + ny - 1) % ny
    p_end, p_mid = x % 2, 1 - x % 2

    load_b = pltpu.make_async_copy(b_hbm, b_v, bload)
    load_b.start()

    def l_slice(t, core):
        return (pl.ds(2 * t * BLOCK, (2 * nt - 2 * t) * BLOCK), pl.ds(pl.multiple_of((2 * t + core) * BLOCK, BLOCK), BLOCK))

    def l_src(t):
        return l_hbm.at[pl.ds(2 * t * BLOCK, (2 * nt - 2 * t) * BLOCK), pl.ds(t * BLOCK, BLOCK)]

    load_l = [pltpu.make_async_copy(l_src(t), l_v.at[l_slice(t, j)], l_sem) for t in range(nt)]
    for copy in load_l:
        copy.start()

    barrier = pltpu.get_barrier_semaphore()
    peers = [at(y, x, 1 - j)] + [at(y, (x + d) % nx) for d in range(1, nx)] + [at(yu, x), at(yd, x)]
    for dev in peers:
        pl.semaphore_signal(barrier, inc=1, device_id=dev, device_id_type=pl.DeviceIdType.MESH)
    load_b.wait()
    pl.semaphore_wait(barrier, len(peers))

    def b_block(m):
        return b_v.at[:, pl.ds(m * BLOCK, BLOCK)]

    s_own = y % 2
    chunk_p, chunk_q = x % 2, x // 2

    def gather_copy(m, yy, i):
        k = ny * m + y
        return remote(b_block(m), b_col.at[k], gsend, grecv.at[k], at(yy, x))

    def pass_copy(m, y_from, y_to, i):
        r = b_col.at[ny * m + y_from]
        return remote(r, r, gsend, grecv.at[ny * m + y_from], at(y_to, x))

    gathers = [gather_copy(0, yu, 0), gather_copy(0, yd, 1), gather_copy(1, yu, 2), gather_copy(1, yd, 3)]
    passes = [pass_copy(1, yd, yu, 4), pass_copy(0, yu, yd, 5)]

    def place_copy(m, d):
        yy = (y + d) % ny
        src = b_col.at[ny * m + yy] if d else b_block(m)
        dst, sem = b_all.at[0, chunk_p, yy % 2, chunk_q], bfirst.at[chunk_p, yy % 2]
        xt = yy // 2 + 2 * m
        return xt, (lambda: remote(src, dst, gsend, sem, at(y, xt))), (lambda: pltpu.make_async_copy(src, dst, sem))

    def came(m, d):
        k = ny * m + (y + d) % ny
        landed(b_col.at[k], grecv.at[k])

    def place(m, d):
        xt, away, here = place_copy(m, d)

        @pl.when(xt != x)
        def _():
            away().start()

        @pl.when(xt == x)
        def _():
            here().start()

    def x_copy(m):
        xt = y // 2 + 2 * (m % 2)
        dst, sem = b_all.at[m // 2, chunk_p, s_own, chunk_q], brecv.at[m // 2 - 1, chunk_p, s_own, chunk_q]
        return xt, (lambda: remote(b_block(m), dst, xsend, sem, at(y, xt))), (lambda: pltpu.make_async_copy(b_block(m), dst, sem))

    def x_first(t):
        for m in (2 * t, 2 * t + 1):
            xt, away, here = x_copy(m)

            @pl.when(xt != x)
            def _():
                away().start()

            @pl.when(xt == x)
            def _():
                here().start()

    is_holder = (y // 2) == (x % 2)
    hx = 2 * (x % 2)
    y_partner = hx + 1 - s_own
    y_outer = (y + ny + 2 * s_own - 1) % ny
    y_next = (y + ny + 1 - 2 * s_own) % ny
    held = is_holder.astype(jnp.int32)
    s_first = held * s_own + (1 - held) * (1 - s_own)

    def y_copy(t, p, s, q, yy):
        r = b_all.at[t, p, s, q]
        return remote(r, r, ysend, brecv.at[t - 1, p, s, q], at(yy, x))

    def b_came(t, p, s, q):
        landed(b_all.at[t, p, s, q], brecv.at[t - 1, p, s, q])

    def forward_held(t, p):
        @pl.when(is_holder)
        def _():
            for q in range(2):
                b_came(t, p, s_own, q)
                y_copy(t, p, s_own, q, y_outer).start()
                y_copy(t, p, s_own, q, y_partner).start()

    def forward_passed(t, p):
        @pl.when(jnp.logical_not(is_holder))
        def _():
            for q in range(2):
                b_came(t, p, 1 - s_own, q)
                y_copy(t, p, 1 - s_own, q, y_next).start()

    def product(p, u, s, m):
        lhs = b_all[u, p, s].reshape(2 * cols, BLOCK)
        rhs = l_v[m * BLOCK:(m + 1) * BLOCK, pl.ds(pl.multiple_of((2 * u + s) * BLOCK, BLOCK), BLOCK)]
        return lax.dot_general(lhs, rhs, (((1,), (1,)), ((), ())), preferred_element_type=F32).reshape(2, cols, BLOCK)

    def await_first(p):
        for s in range(2):
            @pl.when(CORES * x + s <= y + ny)
            def _():
                landed(b_all.at[0, p, s], bfirst.at[p, s])

    def await_rest(p):
        for s in range(2):
            @pl.when(CORES * x + s > y + ny)
            def _():
                landed(b_all.at[0, p, s], bfirst.at[p, s])

    def compute(t, role, sends):
        p = (p_end, p_mid)[role]
        s_last = 1 - s_first
        if t == 0:
            await_first(p)
        if t == 1:
            await_rest(p)
        if role == 0 and t == 0:
            landed(l_v.at[pl.ds(0, (nt + 1) * BLOCK), :], l_sem)
        if t:
            for h in range(2):
                acc = product(p, t, s_first, 2 * t + h)
                for u in range(t):
                    for s in range(2):
                        acc += product(p, u, s, 2 * t + h)
                part[t, role, :, h] = acc
            for q in range(2):
                b_came(t, p, s_last, q)
        for h in range(2):
            m = 2 * t + h
            if t:
                part[t, role, :, h] += product(p, t, s_last, m)
            else:
                part[t, role, :, h] = jnp.zeros((2, cols, BLOCK), F32)
                for s in range(2):
                    @pl.when(CORES * x + s <= y + ny * h)
                    def _():
                        part[t, role, :, h] += product(p, 0, s, m)
            sends[h].start()

    q_own = x // 2

    def far_copy(t, h):
        return remote(part.at[t, 0, 1 - q_own, h], far_in.at[t, h], fsend, far_sem.at[t, h], at(y, xl if h else xr))

    def end_copy(t, side, h):
        xx = xl if side else xr
        return remote(part.at[t, 1, xx // 2, h], end_in.at[t, h, side], esend, end_sem.at[t, h], at(y, xx))

    def ends(t):
        compute(t, 0, [far_copy(t, 0), far_copy(t, 1)])

    def middles(t):
        compute(t, 1, [end_copy(t, 1, 0), end_copy(t, 0, 1)])

    def merge(t, h):
        xx = xl if h else xr
        landed(far_in.at[t, h], far_sem.at[t, h])
        part[t, 1, xx // 2, h] += far_in[t, h]
        end_copy(t, h, h).start()

    def finish(t, h):
        landed(end_in.at[t, h], end_sem.at[t, h])
        m = 2 * t + h
        x_out[:, m * BLOCK:(m + 1) * BLOCK] = (part[t, 0, q_own, h] + (end_in[t, h, 0] + end_in[t, h, 1])).astype(BF16)

    l_copies = [remote(l_src(t), l_v.at[l_slice(t, j)], lsend, l_sem, at(y, x, 1 - j)) for t in range(nt)]
    def start_all(copies):
        for copy in copies:
            copy.start()

    def arrive(m, d, fwd=None):
        came(m, d)
        if fwd is not None:
            passes[fwd].start()
        place(m, d)

    items = {
        "g": lambda: start_all(gathers),
        "p0": lambda: (place(0, 0), place(1, 0)),
        "L": lambda: start_all(l_copies),
        "a01": lambda: arrive(0, 1, 1),
        "a13": lambda: arrive(1, ny - 1, 0),
        "a11": lambda: arrive(1, 1),
        "a03": lambda: arrive(0, ny - 1),
        "a02": lambda: arrive(0, 2),
        "a12": lambda: arrive(1, 2),
    }
    for t in range(1, nt):
        items["x%d" % t] = functools.partial(x_first, t)
        items["he%d" % t] = functools.partial(forward_held, t, p_end)
        items["hm%d" % t] = functools.partial(forward_held, t, p_mid)
        items["fe%d" % t] = functools.partial(forward_passed, t, p_end)
        items["fm%d" % t] = functools.partial(forward_passed, t, p_mid)
    for t in range(nt):
        items["E%d" % t] = functools.partial(ends, t)
        items["M%d" % t] = functools.partial(middles, t)
        items["Ga%d" % t] = functools.partial(merge, t, 0)
        items["Gb%d" % t] = functools.partial(merge, t, 1)
        items["F%d" % t] = lambda t=t: [finish(t, h) for h in range(2)]
    for name in ORDER:
        items[name]()

    landed(l_v.at[pl.ds(0, (nt + 1) * BLOCK // 2), :], lsend)
    landed(b_all.at[:, :, 0], gsend)

    @pl.when(y // 2 == x % 2)
    def _():
        landed(b_v.at[:, pl.ds(0, (nt - 1) * BLOCK)], xsend)
        landed(b_all.at[pl.ds(0, nt - 1)], ysend)

    @pl.when(y // 2 != x % 2)
    def _():
        landed(b_v.at[:, pl.ds(0, 2 * (nt - 1) * BLOCK)], xsend)
        landed(b_all.at[pl.ds(0, nt - 1), :, 0], ysend)

    landed(far_in, fsend)
    for h in range(2):
        finish(nt - 1, h)
    landed(end_in, esend)


def solution(mesh):
    ny = mesh.shape["row"]
    nx = mesh.shape["col"] // CORES

    def local_product(lower_loc, rhs_loc):
        rows, width = lower_loc.shape
        cols = rhs_loc.shape[1]
        nt = width // BLOCK
        dma = pltpu.SemaphoreType.DMA
        return pl.pallas_call(
            functools.partial(kernel, ny, nx, nt),
            out_shape=pltpu.VMEM((cols, rows), BF16),
            in_specs=[pl.BlockSpec(memory_space=pl.ANY)] * 2,
            out_specs=pl.BlockSpec(memory_space=pltpu.VMEM),
            scratch_shapes=[
                pltpu.VMEM((rows, CORES * width), BF16),
                pltpu.VMEM((cols, rows), BF16),
                pltpu.VMEM((2 * ny, cols, BLOCK), BF16),
                pltpu.VMEM((nt, 2, 2, 2, cols, BLOCK), BF16),
                pltpu.VMEM((nt, 2, 2, 2, cols, BLOCK), F32),
                pltpu.VMEM((nt, 2, cols, BLOCK), F32),
                pltpu.VMEM((nt, 2, 2, cols, BLOCK), F32),
                *[dma] * 8, dma((2 * ny,)), dma((2, 2)), dma((nt - 1, 2, 2, 2)), dma((nt, 2)), dma((nt, 2)),
            ],
            compiler_params=pltpu.CompilerParams(collective_id=0, has_side_effects=True),
        )(lower_loc, rhs_loc.T).T

    return jax.shard_map(local_product, mesh=mesh, in_specs=(P("row", "col"), P("row", ("batch", "col"))),
                         out_specs=P("row", ("batch", "col")), check_vma=False)
```
